256 devices in a mesh: blk: 32 (over x, z_lo, y), grp: 8 (over z_hi, core).
Axes of the slice: x: 4, y: 4, z: 8 (z_hi: 4, z_lo: 2; z = z_hi * 2 + z_lo), core: 2. Of those that a mesh axis runs over, the one named last changes fastest.
Arguments:
- points: bfloat16 [64, 32768], P(None, ('blk', 'grp')), may hold values from -6 to 6
- right_side: float32 [16, 32768], P(None, ('blk', 'grp')), may hold values from -18 to 18
- lengthscale: float32 [1], replicated, may hold values from 2.7305508 to 3.3440894
- outputscale: float32 [1], replicated, may hold values from 0.6 to 1.6
- noise_level: float32 [1], replicated, may hold values from 0.4 to 1
Outputs:
- solution: float32 [16, 32768], P(None, ('blk', 'grp'))
- residual: float32 [16, 32768], P(None, ('blk', 'grp'))
- gradient: float32 [3], replicated
The draws below stay inside these ranges and needn't reach their ends.
All inputs are finite; a program needn't handle non-finite values.
Results may differ from the reference program's by a relative error of at most 0.001.
The reference program's roundings to bfloat16 on the way count: a program that leaves them out, or rounds other values in their place, can miss the bound.
Values may be sent and summed in bfloat16 or wider, within the bound.
A program may use at most 64 MiB of HBM per device.

```python
import math
import jax
import jax.numpy as jnp
from jax import lax

DIMS = 64
COLS = 16
ITERS = 2
NPTS = 32768


def draw_points(key, part):
    drawn = jnp.clip(jax.random.normal(key, (DIMS, NPTS), jnp.float32), -6.0, 6.0)
    return drawn.astype(jnp.bfloat16)


def draw_right_side(key, part):
    second_key = jax.random.fold_in(key, 12)
    rising = jnp.exp(math.log(3.0) * jnp.arange(NPTS, dtype=jnp.float32) / max(NPTS - 1, 1))
    drawn = jnp.clip(jax.random.normal(second_key, (COLS, NPTS), jnp.float32), -6.0, 6.0)
    return jnp.clip(drawn * rising[None, :], -18.0, 18.0)


def draw_lengthscale(key, part):
    target = 3.177 * float(NPTS) ** 0.0927
    factor = jax.random.uniform(key, (1,), jnp.float32, 0.9, 1.1)
    return (math.sqrt(10.0 * DIMS) / target * factor).astype(jnp.float32)


def setup_inputs(seed: int = 0) -> dict:
    seeds = jax.random.split(jax.random.key(seed), 6)
    points = draw_points(jax.random.fold_in(seeds[5], 71), 0)
    right_side = draw_right_side(jax.random.fold_in(seeds[5], 71), 0)
    lengthscale = draw_lengthscale(jax.random.fold_in(seeds[5], 71), 0)
    outputscale = jnp.clip(jnp.exp(jax.random.uniform(seeds[3], (1,), jnp.float32, math.log(0.6), math.log(1.6))), 0.6, 1.6)
    noise_level = jnp.clip(jnp.exp(jax.random.uniform(seeds[4], (1,), jnp.float32, math.log(0.4), math.log(1.0))), 0.4, 1.0)
    return {"points": points, "right_side": right_side, "lengthscale": lengthscale, "outputscale": outputscale, "noise_level": noise_level}


def kernel_product(vectors, points_full, squares, scale_len, with_grad):
    rounded = lax.optimization_barrier(vectors.astype(jnp.bfloat16)).astype(jnp.float32)
    block_rows = math.gcd(NPTS, 512)
    block_count = NPTS // block_rows

    def one_block(block_index):
        offset = (block_index * block_rows).astype(jnp.int32)
        row_points = lax.dynamic_slice_in_dim(points_full, offset, block_rows, 1)
        row_squares = lax.dynamic_slice_in_dim(squares, offset, block_rows, 0)
        inner_prod = jnp.dot(row_points.T, points_full, precision=lax.Precision.HIGHEST)
        distance = jnp.maximum(row_squares[:, None] + squares[None, :] - 2.0 * inner_prod, 0.0)
        radius = jnp.sqrt(5.0 * distance) / scale_len
        damping = jnp.exp(-radius)
        kernel_tile = (1.0 + radius + radius * radius / 3.0) * damping
        kernel_tile = lax.optimization_barrier(kernel_tile.astype(jnp.bfloat16)).astype(jnp.float32)
        pieces_out = [jnp.dot(rounded, kernel_tile.T, precision=lax.Precision.HIGHEST)]
        if with_grad:
            slope_tile = radius * radius * (1.0 + radius) * damping / (3.0 * scale_len)
            slope_tile = lax.optimization_barrier(slope_tile.astype(jnp.bfloat16)).astype(jnp.float32)
            pieces_out.append(jnp.dot(rounded, slope_tile.T, precision=lax.Precision.HIGHEST))
        return jnp.concatenate(pieces_out, axis=0)
    stacked = lax.map(one_block, jnp.arange(block_count, dtype=jnp.int32))
    return jnp.moveaxis(stacked, 0, 1).reshape(stacked.shape[1], NPTS)

def reference(points, right_side, lengthscale, outputscale, noise_level):
    points_full = points.astype(jnp.float32)
    squares = lax.optimization_barrier(jnp.sum(points_full * points_full, axis=0))
    scale_len = lengthscale[0]
    amplitude = outputscale[0]
    jitter = noise_level[0]

    def system(vectors):
        return amplitude * kernel_product(vectors, points_full, squares, scale_len, False) + jitter * vectors
    solution = jnp.zeros_like(right_side)
    residual = right_side
    direction = right_side
    norm_now = lax.optimization_barrier(jnp.sum(residual * residual, axis=1))
    for iteration in range(ITERS):
        applied = system(direction)
        curvature = lax.optimization_barrier(jnp.sum(direction * applied, axis=1))
        step_size = norm_now / curvature
        solution = solution + step_size[:, None] * direction
        residual = residual - step_size[:, None] * applied
        if iteration + 1 < ITERS:
            norm_next = lax.optimization_barrier(jnp.sum(residual * residual, axis=1))
            direction = residual + (norm_next / norm_now)[:, None] * direction
            norm_now = norm_next
    products_out = kernel_product(solution, points_full, squares, scale_len, True)
    kernel_part = products_out[:COLS]
    slope_part = products_out[COLS:]
    left_side = jnp.concatenate([solution[:1], right_side[1:]], axis=0)
    weights = jnp.where(jnp.arange(COLS, dtype=jnp.int32) == 0, 1.0, -1.0 / (COLS - 1)).astype(jnp.float32)[:, None]
    local_terms = jnp.stack([jnp.sum(weights * left_side * amplitude * slope_part), jnp.sum(weights * left_side * kernel_part), jnp.sum(weights * left_side * solution)])
    gradient = 0.5 * local_terms / NPTS
    return (solution, residual, gradient)
```

```python
import math

import jax
import jax.numpy as jnp
from jax import lax
from jax.experimental import pallas as pl
from jax.experimental.pallas import tpu as pltpu
from jax.sharding import Mesh
from jax.sharding import PartitionSpec as P

AXES = ("x", "zl", "y", "zh", "c")
BY_ID = pl.DeviceIdType.MESH
F32 = jnp.float32
BF16 = jnp.bfloat16
DEPTH = 80


def add_all(terms):
    total = terms[0]
    for term in terms[1:]:
        total = total + term
    return total


def make_kernel(sizes, columns, width, total_points):
    xs, zls, ys, zhs, cs = sizes
    zs, gs = zls * zhs, ys * cs
    half = zs // 2
    x_tiles, row_tiles = zs // 2, gs // 2
    tiles = xs * x_tiles
    copies_in_all = 4 * (zs - 1) + 8 * (gs - 1) + 18 + (xs - 1)

    def kernel(
        points,
        right,
        length_ref,
        scale_ref,
        noise_ref,
        solution_out,
        residual_out,
        gradient_out,
        cols,
        r0c,
        a1c,
        rows,
        r0r,
        a1r,
        d2r,
        weights,
        kmat,
        gmat,
        acc,
        vb2,
        rs1,
        rs2,
        ex1,
        ex2,
        fin_g,
        fin_z,
        fin_x,
        send_sems,
        recv_sems,
    ):
        x, y, c = lax.axis_index("x"), lax.axis_index("y"), lax.axis_index("c")
        z = lax.axis_index("zh") * zls + lax.axis_index("zl")

        def z_peer(k):
            to = lax.rem(z + k, zs)
            return {"zl": lax.rem(to, zls), "zh": lax.div(to, zls)}

        def g_peer(dy, dc):
            return {"y": lax.rem(y + dy, ys), "c": lax.rem(c + dc, cs)}

        def x_peer(k):
            return {"x": lax.rem(x + k, xs)}

        started = []

        def send(src, dst, device):
            index = len(started)
            copy = pltpu.make_async_remote_copy(
                src_ref=src,
                dst_ref=dst,
                send_sem=send_sems.at[index],
                recv_sem=recv_sems.at[index],
                device_id=device,
                device_id_type=BY_ID,
            )
            copy.start()
            started.append(copy)
            return copy

        def to_z(src, slots):
            return [send(src, slots(k), z_peer(k)) for k in range(1, zs)]

        def to_g(src, slots):
            return [send(src, slots(s), g_peer(s // cs, s % cs)) for s in range(1, gs)]

        def scatter_g(source, slots):
            return [
                send(source(s), slots(((ys - s // cs) % ys) * cs + s % cs), g_peer(ys - s // cs, s % cs))
                for s in range(1, gs)
            ]

        def wait(copies):
            for copy in copies:
                copy.wait_recv()

        own = points[...].astype(F32)
        norm = jnp.sum(own * own, axis=0, keepdims=True)
        high = norm.astype(BF16).astype(F32)
        middle = (norm - high).astype(BF16).astype(F32)
        low = norm - high - middle
        line = lax.broadcasted_iota(jnp.int32, (DEPTH - 64, width), 0)
        pieces = jnp.where(line % 3 == 0, high, jnp.where(line % 3 == 1, middle, low))
        first, second = line < 3, (line >= 3) & (line < 6)
        cols[0, 0, 0:64, :] = points[...]
        cols[0, 0, 64:DEPTH, :] = jnp.where(first, pieces, jnp.where(second, 1.0, 0.0)).astype(BF16)
        rows[0, 0:64, :] = (own * -2.0).astype(BF16)
        rows[0, 64:DEPTH, :] = jnp.where(first, 1.0, jnp.where(second, pieces, 0.0)).astype(BF16)
        r0c[0, 0] = right[...]
        r0r[0] = right[...]
        acc[0] = jnp.zeros_like(acc[0])
        acc[1] = jnp.zeros_like(acc[1])

        barrier = pltpu.get_barrier_semaphore()
        peers = [z_peer(k) for k in range(1, zs)] + [g_peer(s // cs, s % cs) for s in range(1, gs)]
        peers += [x_peer(k) for k in range(1, xs)]
        for peer in peers:
            pl.semaphore_signal(barrier, inc=1, device_id=peer, device_id_type=BY_ID)
        pl.semaphore_wait(barrier, len(peers))

        z_cols = to_z(cols.at[0, 0], lambda k: cols.at[0, k])
        g_rows = to_g(rows.at[0], lambda s: rows.at[s])
        z_r0 = to_z(r0c.at[0, 0], lambda k: r0c.at[0, k])
        g_r0 = to_g(r0r.at[0], lambda s: r0r.at[s])

        inv = jnp.max(1.0 / jnp.full((8, 128), length_ref[0], F32))
        root = inv * math.sqrt(5.0)
        rate = inv * (-math.sqrt(5.0) / math.log(2.0))
        third = inv * inv * (5.0 / 3.0)
        slope = inv * inv * inv * (5.0 / 3.0)
        amplitude, jitter = scale_ref[0], noise_ref[0]

        def kernel_pair(inner):
            dist = jnp.maximum(inner, 1e-30)
            root_dist = dist * lax.rsqrt(dist)
            damping = jnp.exp2(root_dist * rate)
            linear = root_dist * root + 1.0
            kern = (linear + dist * third) * damping
            dkern = (dist * slope) * linear * damping
            return kern.astype(BF16), dkern.astype(BF16)

        def add_product(which, part, r, product):
            acc[which, part, 2 * r] += product[:, :width]
            acc[which, part, 2 * r + 1] += product[:, width:]

        def sweep(slot, low_tile, high_tile):
            def one_tile(t, carry):
                padding = jnp.zeros((128 - DEPTH, width), F32)
                turned = [
                    jnp.transpose(jnp.concatenate([cols[slot, 2 * t + h].astype(F32), padding], axis=0)).astype(BF16)
                    for h in range(2)
                ]
                turned = jnp.concatenate(turned, axis=0)
                vectors = jnp.concatenate([r0c[slot, 2 * t], r0c[slot, 2 * t + 1]], axis=1).astype(BF16)
                at = slot * x_tiles + t
                for r in range(row_tiles):
                    inner = jnp.dot(turned, weights[r], preferred_element_type=F32)
                    for q in range(0, 2 * width, 32):
                        kern, dkern = kernel_pair(inner[q : q + 32])
                        kmat[at, r, q : q + 32, :] = kern
                        gmat[at, r, q : q + 32, :] = dkern
                    add_product(0, 0, r, jnp.dot(vectors, kmat[at, r], preferred_element_type=F32))
                    add_product(0, 1, r, jnp.dot(vectors, gmat[at, r], preferred_element_type=F32))
                return carry

            lax.fori_loop(low_tile, high_tile, one_tile, 0)

        def start_ring(buffers):
            moves = {}
            for h in range(2):
                part = pl.ds(h * half, half)
                moves["right", h] = [send(b.at[0, part], b.at[1, part], x_peer(1)) for b in buffers]
            for h in (1, 0):
                part = pl.ds(h * half, half)
                moves["left", h] = [send(b.at[0, part], b.at[2, part], x_peer(xs - 1)) for b in buffers]
            return moves

        def pass_on(moves, buffers):
            wait(moves["right", 0])
            moves["far", 0] = [send(b.at[1, pl.ds(0, half)], b.at[3, pl.ds(0, half)], x_peer(1)) for b in buffers]
            wait(moves["left", 1])
            moves["far", 1] = [
                send(b.at[2, pl.ds(half, half)], b.at[3, pl.ds(half, half)], x_peer(xs - 1)) for b in buffers
            ]

        wait(z_cols + z_r0)
        ring = start_ring([cols, r0c])
        wait(g_rows)
        for r in range(row_tiles):
            weights[r, 0:DEPTH, :] = jnp.concatenate([rows[2 * r], rows[2 * r + 1]], axis=1)
            weights[r, DEPTH:128, :] = jnp.zeros((128 - DEPTH, 2 * width), BF16)
        mid = x_tiles // 2
        sweep(0, 0, x_tiles)
        pass_on(ring, [cols, r0c])
        sweep(1, 0, mid)
        sweep(2, mid, x_tiles)
        wait(ring["right", 1])
        sweep(1, mid, x_tiles)
        wait(ring["left", 0])
        sweep(2, 0, mid)
        wait(ring["far", 0])
        sweep(3, 0, mid)
        wait(ring["far", 1])
        sweep(3, mid, x_tiles)

        arriving = scatter_g(lambda s: acc.at[0, 0, s], lambda s: rs1.at[s])
        wait(arriving)
        product = add_all([acc[0, 0, 0]] + [rs1[s] for s in range(1, gs)])
        applied = amplitude * product + jitter * right[...]
        a1c[0, 0] = applied
        a1r[0] = applied
        z_a1 = to_z(a1c.at[0, 0], lambda k: a1c.at[0, k])
        g_a1 = to_g(a1r.at[0], lambda s: a1r.at[s])
        wait(z_a1)
        ring = start_ring([a1c])
        pass_on(ring, [a1c])
        wait(ring["right", 1] + ring["left", 0] + ring["far", 0] + ring["far", 1])

        lane = lax.broadcasted_iota(jnp.int32, (columns, width), 1)

        def pack(sums):
            tile = jnp.zeros((columns, width), F32)
            for index, value in enumerate(sums):
                tile = jnp.where(lane == index, jnp.sum(value, axis=1, keepdims=True), tile)
            return tile

        def take(tile, index):
            return jnp.sum(jnp.where(lane == index, tile, 0.0), axis=1, keepdims=True)

        units = [(i, k) for i in range(xs) for k in range(zs)]
        ex1[0] = pack(
            [add_all([r0c[u] * r0c[u] for u in units]), add_all([r0c[u] * a1c[u] for u in units])]
        )
        wait(to_g(ex1.at[0], lambda s: ex1.at[s]))
        total = add_all([ex1[s] for s in range(gs)])
        rr0, curvature = take(total, 0), take(total, 1)
        step1 = rr0 / curvature

        def new_residual(u):
            return r0c[u] - step1 * a1c[u]

        ex2[0] = pack([add_all([new_residual(u) * new_residual(u) for u in units])])
        wait(to_g(ex2.at[0], lambda s: ex2.at[s]))
        rr1 = take(add_all([ex2[s] for s in range(gs)]), 0)
        ratio = rr1 / rr0
        for i in range(xs):
            for t in range(x_tiles):
                pair = [new_residual((i, 2 * t + h)) + ratio * r0c[i, 2 * t + h] for h in range(2)]
                vb2[i * x_tiles + t] = jnp.concatenate(pair, axis=1).astype(BF16)

        def second_product(part, mat):
            def one_tile(t, carry):
                for r in range(row_tiles):
                    add_product(1, part, r, jnp.dot(vb2[t], mat[t, r], preferred_element_type=F32))
                return carry

            lax.fori_loop(0, tiles, one_tile, 0)

        second_product(0, kmat)
        arriving = scatter_g(lambda s: acc.at[1, 0, s], lambda s: rs2.at[s])
        second_product(1, gmat)

        wait(g_a1 + g_r0)
        for s in range(gs):
            d2r[s] = (r0r[s] - step1 * a1r[s]) + ratio * r0r[s]
        sums = []
        for left in (r0r, d2r):
            for which in range(2):
                for part in range(2):
                    sums.append(add_all([left[s] * acc[which, part, s] for s in range(gs)]))
        sums += [r0r[0] * d2r[0], d2r[0] * d2r[0]]
        fin_g[0] = pack(sums)
        wait(to_g(fin_g.at[0], lambda s: fin_g.at[s]))
        fin_z[0] = add_all([fin_g[s] for s in range(gs)])
        wait(to_z(fin_z.at[0], lambda k: fin_z.at[k]))
        fin_x[0] = add_all([fin_z[k] for k in range(zs)])
        wait([send(fin_x.at[0], fin_x.at[k], x_peer(k)) for k in range(1, xs)])
        total = add_all([fin_x[k] for k in range(xs)])
        (r0_k1, r0_g1, r0_k2, r0_g2, d2_k1, d2_g1, d2_k2, d2_g2, r0_d2, d2_d2) = [take(total, i) for i in range(10)]

        step2 = rr1 / (amplitude * d2_k2 + jitter * d2_d2)
        wait(arriving)
        product = add_all([acc[1, 0, 0]] + [rs2[s] for s in range(1, gs)])
        applied = amplitude * product + jitter * d2r[0]
        solution_out[...] = step1 * right[...] + step2 * d2r[0]
        residual_out[...] = (right[...] - step1 * a1r[0]) - step2 * applied

        top = lax.broadcasted_iota(jnp.int32, (columns, 1), 0) == 0
        weight = jnp.where(top, 1.0, -1.0 / (columns - 1))

        def quadratic(r0_r0, r0_d2, d2_r0, d2_d2):
            plain = step1 * r0_r0 + step2 * r0_d2
            other = step1 * d2_r0 + step2 * d2_d2
            return jnp.sum(weight * jnp.where(top, step1 * plain + step2 * other, plain))

        share = 0.5 / total_points
        gradient_out[0] = quadratic(r0_g1, r0_g2, d2_g1, d2_g2) * amplitude * share
        gradient_out[1] = quadratic(r0_k1, r0_k2, d2_k1, d2_k2) * share
        gradient_out[2] = quadratic(rr0, r0_d2, r0_d2, d2_d2) * share

        assert len(started) == copies_in_all
        for copy in started:
            copy.wait_send()

    unit = (columns, width)
    scratch = [
        pltpu.VMEM((xs, zs, DEPTH, width), BF16),
        pltpu.VMEM((xs, zs, *unit), F32),
        pltpu.VMEM((xs, zs, *unit), F32),
        pltpu.VMEM((gs, DEPTH, width), BF16),
        pltpu.VMEM((gs, *unit), F32),
        pltpu.VMEM((gs, *unit), F32),
        pltpu.VMEM((gs, *unit), F32),
        pltpu.VMEM((row_tiles, 128, 2 * width), BF16),
        pltpu.VMEM((tiles, row_tiles, 2 * width, 2 * width), BF16),
        pltpu.VMEM((tiles, row_tiles, 2 * width, 2 * width), BF16),
        pltpu.VMEM((2, 2, gs, *unit), F32),
        pltpu.VMEM((tiles, columns, 2 * width), BF16),
        pltpu.VMEM((gs, *unit), F32),
        pltpu.VMEM((gs, *unit), F32),
        pltpu.VMEM((gs, *unit), F32),
        pltpu.VMEM((gs, *unit), F32),
        pltpu.VMEM((gs, *unit), F32),
        pltpu.VMEM((zs, *unit), F32),
        pltpu.VMEM((xs, *unit), F32),
        pltpu.SemaphoreType.DMA((copies_in_all,)),
        pltpu.SemaphoreType.DMA((copies_in_all,)),
    ]
    vmem = pl.BlockSpec(memory_space=pltpu.VMEM)
    smem = pl.BlockSpec(memory_space=pltpu.SMEM)
    return pl.pallas_call(
        kernel,
        out_shape=(
            jax.ShapeDtypeStruct(unit, F32),
            jax.ShapeDtypeStruct(unit, F32),
            jax.ShapeDtypeStruct((3,), F32),
        ),
        in_specs=[vmem, vmem, smem, smem, smem],
        out_specs=(vmem, vmem, smem),
        scratch_shapes=scratch,
        compiler_params=pltpu.CompilerParams(
            collective_id=0, has_side_effects=True, vmem_limit_bytes=48 * 1024 * 1024
        ),
    )


def solution(mesh):
    sizes = (4, 2, 4, 4, 2)
    split = Mesh(mesh.devices.reshape(sizes), AXES)

    def local(points, right_side, lengthscale, outputscale, noise_level):
        columns, width = right_side.shape
        call = make_kernel(sizes, columns, width, width * math.prod(sizes))
        return call(points, right_side, lengthscale, outputscale, noise_level)

    return jax.shard_map(
        local,
        mesh=split,
        in_specs=(P(None, AXES), P(None, AXES), P(), P(), P()),
        out_specs=(P(None, AXES), P(None, AXES), P()),
        check_vma=False,
    )
```

```python
import math

import jax
import jax.numpy as jnp
from jax import lax
from jax.experimental import pallas as pl
from jax.experimental.pallas import tpu as pltpu
from jax.sharding import Mesh
from jax.sharding import PartitionSpec as P

AXES = ("x", "zl", "y", "zh", "c")
BY_ID = pl.DeviceIdType.MESH
F32 = jnp.float32
BF16 = jnp.bfloat16
FEATURES = 64
UNIT = 80


def add_all(terms):
    total = terms[0]
    for term in terms[1:]:
        total = total + term
    return total


def two_sum(a, b):
    s = a + b
    t = s - a
    return s, (a - (s - t)) + (b - t)


def pair_sum(a, b):
    s, e = two_sum(a[0], b[0])
    e = e + (a[1] + b[1])
    high = s + e
    return high, e - (high - s)


def halves(a):
    t = a * 4097.0
    high = t - (t - a)
    return high, a - high


def two_product(a, b):
    p = a * b
    (ah, al), (bh, bl) = halves(a), halves(b)
    return p, ((ah * bh - p) + ah * bl + al * bh) + al * bl


def pair_tree(pairs):
    while len(pairs) > 1:
        pairs = [pair_sum(pairs[i], pairs[i + 1]) for i in range(0, len(pairs), 2)]
    return pairs[0]


def make_kernel(sizes, columns, width, total_points):
    xs, zls, ys, zhs, cs = sizes
    zs, gs = zls * zhs, ys * cs
    planes = xs * gs
    half = zs // 2
    x_tiles, row_tiles = zs // 2, gs // 2
    tiles = xs * x_tiles
    wide = 2 * width
    copies_in_all = 3 * (zs - 1) + 5 * (gs - 1) + 18 + 2 * (planes - 1 + zs - 1)
    z_offsets = [0] + [k for d in range(1, half) for k in (d, zs - d)] + [half]

    def kernel(
        points_in,
        right_in,
        length_in,
        scale_in,
        noise_in,
        solution_out,
        residual_out,
        gradient_out,
        cols,
        r0c,
        a1c,
        rows,
        r0r,
        a1r,
        d2r,
        weights,
        kmat,
        gmat,
        acc,
        vb2,
        upright,
        rs1,
        rs2,
        plane1,
        line1,
        plane2,
        line2,
        local_sems,
        send_sems,
        recv_sems,
    ):
        x, y, c = lax.axis_index("x"), lax.axis_index("y"), lax.axis_index("c")
        z = lax.axis_index("zh") * zls + lax.axis_index("zl")

        def z_peer(k):
            to = lax.rem(z + k, zs)
            return {"zl": lax.rem(to, zls), "zh": lax.div(to, zls)}

        def plane_peer(s):
            dx, dy, dc = s // gs, s % gs // cs, s % cs
            return {"x": lax.rem(x + dx, xs), "y": lax.rem(y + dy, ys), "c": lax.rem(c + dc, cs)}

        def x_peer(k):
            return {"x": lax.rem(x + k, xs)}

        barrier = pltpu.get_barrier_semaphore()
        peers = [z_peer(k) for k in range(1, zs)] + [plane_peer(s) for s in range(1, planes)]
        for peer in peers:
            pl.semaphore_signal(barrier, inc=1, device_id=peer, device_id_type=BY_ID)

        fetches = [
            pltpu.make_async_copy(src, dst, local_sems.at[i])
            for i, (src, dst) in enumerate(
                [
                    (right_in, r0c.at[0, 0]),
                    (right_in, r0r.at[0]),
                    (points_in, cols.at[0, 0, pl.ds(0, FEATURES)]),
                    (points_in, rows.at[0]),
                ]
            )
        ]
        for fetch in fetches:
            fetch.start()
        started = []

        def send(src, dst, device):
            index = len(started)
            copy = pltpu.make_async_remote_copy(
                src_ref=src,
                dst_ref=dst,
                send_sem=send_sems.at[index],
                recv_sem=recv_sems.at[index],
                device_id=device,
                device_id_type=BY_ID,
            )
            copy.start()
            started.append(copy)
            return copy

        def to_z(src, slots):
            return [send(src, slots(j), z_peer(z_offsets[j])) for j in range(1, zs)]

        def to_g(src, slots):
            return [send(src, slots(s), plane_peer(s)) for s in range(1, gs)]

        def opposite(s):
            return ((ys - s // cs) % ys) * cs + s % cs

        def wait(copies):
            for copy in copies:
                copy.wait_recv()

        acc[...] = jnp.zeros_like(acc)
        for r in range(row_tiles):
            weights[r, UNIT:128, :] = jnp.zeros((128 - UNIT, wide), BF16)
        for fetch in fetches:
            fetch.wait()
        r0 = r0c[0, 0]
        cols[0, 0, FEATURES:UNIT, :] = r0.astype(BF16)
        pl.semaphore_wait(barrier, len(peers))

        z_cols = to_z(cols.at[0, 0], lambda j: cols.at[0, j])
        g_rows = to_g(rows.at[0], lambda s: rows.at[s])
        inv = jnp.max(1.0 / jnp.full((8, 128), length_in[0], F32))
        root = inv * math.sqrt(5.0)
        rate = inv * (-math.sqrt(5.0) / math.log(2.0))
        third = inv * inv * (5.0 / 3.0)
        amplitude, jitter = scale_in[0], noise_in[0]

        line = lax.broadcasted_iota(jnp.int32, (16, width), 0)
        first, second = line < 3, (line >= 3) & (line < 6)

        def norm_pieces(values):
            norm = jnp.sum(values * values, axis=0, keepdims=True)
            high = norm.astype(BF16).astype(F32)
            middle = (norm - high).astype(BF16).astype(F32)
            low = norm - high - middle
            return jnp.where(line % 3 == 0, high, jnp.where(line % 3 == 1, middle, low))

        def column_side(unit):
            values = unit.astype(F32)
            extra = jnp.where(first, norm_pieces(values), jnp.where(second, 1.0, 0.0))
            padding = jnp.zeros((128 - UNIT, width), F32)
            return jnp.transpose(jnp.concatenate([values, extra, padding], axis=0)).astype(BF16)

        def row_side(unit):
            values = unit.astype(F32)
            extra = jnp.where(first, 1.0, jnp.where(second, norm_pieces(values), 0.0))
            return jnp.concatenate([values * -2.0, extra], axis=0).astype(BF16)

        def kernel_pair(inner):
            dist = jnp.maximum(inner, 1e-30)
            root_dist = dist * lax.rsqrt(dist)
            damping = jnp.exp2(root_dist * rate)
            linear = root_dist * root + 1.0
            bend = dist * third
            plain = linear * damping
            return (plain + bend * damping).astype(BF16), (bend * plain).astype(BF16)

        def add_product(part, r, product):
            acc[part, 2 * r] += product[:, :width]
            acc[part, 2 * r + 1] += product[:, width:]

        def load_tile(slot, t):
            turned = [column_side(cols[slot, 2 * t + h, 0:FEATURES, :]) for h in range(2)]
            vectors = [cols[slot, 2 * t + h, FEATURES:UNIT, :] for h in range(2)]
            return jnp.concatenate(turned, axis=0), jnp.concatenate(vectors, axis=1)

        def one_block(at, r, turned, vectors):
            inner = jnp.dot(turned, weights[r], preferred_element_type=F32)
            for q in range(0, wide, 32):
                kern, dkern = kernel_pair(inner[q : q + 32])
                kmat[r, at, q : q + 32, :] = kern
                gmat[r, at, q : q + 32, :] = dkern
            add_product(0, r, jnp.dot(vectors, kmat[r, at], preferred_element_type=F32))
            add_product(1, r, jnp.dot(vectors, gmat[r, at], preferred_element_type=F32))

        def sweep(slot, low_tile, high_tile):
            def one_tile(t, carry):
                turned, vectors = load_tile(slot, t)
                for r in range(row_tiles):
                    one_block(slot * x_tiles + t, r, turned, vectors)
                return carry

            lax.fori_loop(low_tile, high_tile, one_tile, 0)

        def ring_send(buf, h, slot, way):
            part = pl.ds(h * half, half)
            return [send(buf.at[0, part], buf.at[slot, part], x_peer(way))]

        def ring_rest(buf, ring):
            ring["right", 1] = ring_send(buf, 1, 1, 1)
            ring["left", 1] = ring_send(buf, 1, 2, xs - 1)
            ring["left", 0] = ring_send(buf, 0, 2, xs - 1)

        def pass_right(buf, ring):
            wait(ring["right", 0])
            part = pl.ds(0, half)
            ring["far", 0] = [send(buf.at[1, part], buf.at[3, part], x_peer(1))]

        def pass_left(buf, ring):
            wait(ring["left", 1])
            part = pl.ds(half, half)
            ring["far", 1] = [send(buf.at[2, part], buf.at[3, part], x_peer(xs - 1))]

        mid = x_tiles // 2
        wait(g_rows)
        for r in range(row_tiles):
            weights[r, 0:UNIT, :] = jnp.concatenate([row_side(rows[2 * r]), row_side(rows[2 * r + 1])], axis=1)
        ring = {}
        wait(z_cols[: half - 1])
        ring["right", 0] = ring_send(cols, 0, 1, 1)
        sweep(0, 0, mid)
        wait(z_cols[half - 1 :])
        ring_rest(cols, ring)
        z_r0 = to_z(r0c.at[0, 0], lambda j: r0c.at[0, j])
        g_r0 = to_g(r0r.at[0], lambda s: r0r.at[s])
        sweep(0, mid, x_tiles)
        pass_right(cols, ring)
        sweep(1, 0, mid)
        pass_left(cols, ring)
        sweep(2, mid, x_tiles)
        wait(ring["right", 1])
        sweep(1, mid, x_tiles)
        wait(z_r0)
        ring0 = {("right", 0): ring_send(r0c, 0, 1, 1)}
        ring_rest(r0c, ring0)
        wait(ring["left", 0])
        sweep(2, 0, mid)
        wait(ring["far", 0])
        sweep(3, 0, mid)
        pass_right(r0c, ring0)
        pass_left(r0c, ring0)
        wait(ring["far", 1])

        order = [r for r in range(1, row_tiles)] + [0]
        loaded = [load_tile(3, t) for t in range(mid, x_tiles)]
        arriving = []
        for r in order:
            for t in range(mid, x_tiles):
                one_block(3 * x_tiles + t, r, *loaded[t - mid])
            for s in (2 * r, 2 * r + 1):
                if s:
                    arriving.append(send(acc.at[0, s], rs1.at[opposite(s)], plane_peer(opposite(s))))
        wait(arriving)
        product = add_all([acc[0, 0]] + [rs1[s] for s in range(1, gs)])
        a1 = amplitude * product + jitter * r0
        a1c[0, 0] = a1
        a1r[0] = a1
        z_a1 = to_z(a1c.at[0, 0], lambda j: a1c.at[0, j])
        g_a1 = to_g(a1r.at[0], lambda s: a1r.at[s])

        lane = lax.broadcasted_iota(jnp.int32, (8, 128), 1)

        def stack(parts):
            parts = list(parts) + [jnp.zeros((128 - columns * len(parts), width), F32)] * (columns * len(parts) < 128)
            return jnp.transpose(jnp.concatenate(parts, axis=0))

        def unstack(row):
            turned = jnp.transpose(jnp.broadcast_to(row[0:1], (128, 128)))
            return [turned[columns * i : columns * (i + 1)] for i in range(128 // columns)]

        def sublane_pair(pair):
            for shift in (4, 2, 1):
                pair = pair_sum(pair, tuple(pltpu.roll(v, shift, 0) for v in pair))
            return pair

        def join(pair):
            return jnp.where(lane < 64, pair[0], pltpu.roll(pair[1], 64, 1))

        def split(row):
            return row, pltpu.roll(row, 64, 1)

        def eights(buf, count):
            return [jnp.concatenate([buf[i + j] for j in range(8)], axis=0) for i in range(0, count, 8)]

        def pair_total(buf, count):
            return sublane_pair(pair_tree([split(rows8) for rows8 in eights(buf, count)]))

        products = [two_product(r0, r0), two_product(r0, a1), two_product(a1, a1)]
        high, low = stack([p for p, _ in products]), stack([e for _, e in products])
        own_sums = sublane_pair(pair_tree([(high[i : i + 8], low[i : i + 8]) for i in range(0, 128, 8)]))
        plane1[0] = join(own_sums)[0:1]
        in_plane = [send(plane1.at[0], plane1.at[s], plane_peer(s)) for s in range(1, planes)]

        ring = {}
        wait(z_a1[: half - 1])
        ring["right", 0] = ring_send(a1c, 0, 1, 1)
        wait(z_a1[half - 1 :])
        ring_rest(a1c, ring)
        wait(in_plane)
        line1[0] = join(pair_total(plane1, planes))[0:1]
        in_line = [send(line1.at[0], line1.at[k], z_peer(k)) for k in range(1, zs)]
        pass_right(a1c, ring)
        pass_left(a1c, ring)
        wait(g_a1 + g_r0)
        wait(ring0["right", 1] + ring0["left", 0] + ring0["far", 0] + ring0["far", 1])
        wait(in_line)
        sums = pair_total(line1, zs)

        def aligned(i):
            return tuple(pltpu.roll(v, (128 - columns * i) % 128, 1) if i else v for v in sums)

        rr0_pair, curve_pair, aa_pair = aligned(0), aligned(1), aligned(2)
        step1_row = rr0_pair[0] / curve_pair[0]
        cross, cross_low = two_product(curve_pair[0], -2.0 * step1_row)
        cross = (cross, cross_low - 2.0 * step1_row * curve_pair[1])
        square, square_low = two_product(step1_row, step1_row)
        bend, bend_low = two_product(aa_pair[0], square)
        bend = (bend, bend_low + (aa_pair[0] * square_low + aa_pair[1] * square))
        rr1_pair = pair_sum(pair_sum(rr0_pair, cross), bend)
        rr1_row = rr1_pair[0] + rr1_pair[1]
        packed = step1_row
        for i, row in enumerate((rr1_row / rr0_pair[0], rr1_row, rr0_pair[0])):
            packed = jnp.where(lane >= columns * (i + 1), pltpu.roll(row, columns * (i + 1), 1), packed)
        step1, ratio, rr1, rr0 = unstack(packed)[:4]
        wait(ring["right", 1] + ring["left", 0] + ring["far", 0] + ring["far", 1])

        def new_direction(r0_part, a1_part):
            return (r0_part - step1 * a1_part) + ratio * r0_part

        for i in range(xs):
            for t in range(x_tiles):
                pair = [new_direction(r0c[i, 2 * t + h], a1c[i, 2 * t + h]) for h in range(2)]
                at = i * x_tiles + t
                side, place = at // (tiles // 2), at % (tiles // 2) * wide
                vb2[side, :, place : place + wide] = jnp.concatenate(pair, axis=1).astype(BF16)
                for h in range(2):
                    upright[i * x_tiles + t, h * width : (h + 1) * width, :] = jnp.transpose(
                        jnp.broadcast_to(pair[h][0:1], (width, width))
                    )
        for s in range(gs):
            d2r[s] = new_direction(r0r[s], a1r[s])
        d2 = d2r[0]

        arriving = []
        bilinear = jnp.zeros((16, width), F32)
        for r in order:
            sides = []
            slopes = jnp.zeros((16, wide), F32)
            for side in range(2):
                part = kmat[r, side * (tiles // 2) : (side + 1) * (tiles // 2)].reshape(tiles // 2 * wide, wide)
                sides.append(jnp.dot(vb2[side], part, preferred_element_type=F32))
            for t in range(tiles):
                for q in range(0, wide, 64):
                    scale = upright[t, q : q + 64, :]
                    terms = gmat[r, t, q : q + 64, :].astype(F32) * jnp.concatenate([scale, scale], axis=1)
                    slopes = slopes + add_all([terms[i : i + 16] for i in range(0, 64, 16)])
            total = sides[0] + sides[1]
            for h in range(2):
                s = 2 * r + h
                acc[2, s] = total[:, h * width : (h + 1) * width]
                bilinear = bilinear + slopes[:, h * width : (h + 1) * width] * d2r[s][0:1]
                if s:
                    arriving.append(send(acc.at[2, s], rs2.at[opposite(s)], plane_peer(opposite(s))))

        def dot_rows(left, part):
            return add_all([left[s] * acc[part, s] for s in range(gs)])

        top = lax.broadcasted_iota(jnp.int32, (columns, width), 0) == 0
        slope_rows = jnp.where(top, jnp.sum(bilinear, axis=0, keepdims=True), 0.0)
        stats = [dot_rows(r0r, 0), dot_rows(r0r, 1), dot_rows(d2r, 1), slope_rows]
        stats += [dot_rows(r0r, 2), dot_rows(d2r, 2), r0 * d2, d2 * d2]
        plane2[0] = jnp.sum(stack(stats), axis=0, keepdims=True)
        wait([send(plane2.at[0], plane2.at[s], plane_peer(s)) for s in range(1, planes)])
        line2[0] = jnp.sum(add_all(eights(plane2, planes)), axis=0, keepdims=True)
        wait([send(line2.at[0], line2.at[k], z_peer(k)) for k in range(1, zs)])
        total = jnp.sum(add_all(eights(line2, zs)), axis=0, keepdims=True)
        r0_k1, r0_g1, d2_g1, d2_g2, r0_k2, d2_k2, r0_d2, d2_d2 = unstack(total)

        step2 = rr1 / (amplitude * d2_k2 + jitter * d2_d2)
        wait(arriving)
        product = add_all([acc[2, 0]] + [rs2[s] for s in range(1, gs)])
        applied = amplitude * product + jitter * d2
        solution_out[...] = step1 * r0 + step2 * d2
        residual_out[...] = (r0 - step1 * a1) - step2 * applied

        weight = jnp.where(top, 1.0, -1.0 / (columns - 1))

        def quadratic(r0_r0, mixed, d2_d2):
            plain = step1 * r0_r0 + step2 * mixed
            other = step1 * mixed + step2 * d2_d2
            terms = weight * jnp.where(top, step1 * plain + step2 * other, plain)
            return jnp.sum(terms[:, 0:1])

        share = 0.5 / total_points
        gradient_out[0] = quadratic(r0_g1, d2_g1, d2_g2) * amplitude * inv * share
        gradient_out[1] = quadratic(r0_k1, r0_k2, d2_k2) * share
        gradient_out[2] = quadratic(rr0, r0_d2, d2_d2) * share

        assert len(started) == copies_in_all, len(started)
        for copy in started:
            copy.wait_send()

    unit = (columns, width)
    scratch = [
        pltpu.VMEM((xs, zs, UNIT, width), BF16),
        pltpu.VMEM((xs, zs, *unit), F32),
        pltpu.VMEM((xs, zs, *unit), F32),
        pltpu.VMEM((gs, FEATURES, width), BF16),
        pltpu.VMEM((gs, *unit), F32),
        pltpu.VMEM((gs, *unit), F32),
        pltpu.VMEM((gs, *unit), F32),
        pltpu.VMEM((row_tiles, 128, wide), BF16),
        pltpu.VMEM((row_tiles, tiles, wide, wide), BF16),
        pltpu.VMEM((row_tiles, tiles, wide, wide), BF16),
        pltpu.VMEM((3, gs, *unit), F32),
        pltpu.VMEM((2, columns, tiles // 2 * wide), BF16),
        pltpu.VMEM((tiles, wide, width), F32),
        pltpu.VMEM((gs, *unit), F32),
        pltpu.VMEM((gs, *unit), F32),
        pltpu.VMEM((planes, 1, 128), F32),
        pltpu.VMEM((zs, 1, 128), F32),
        pltpu.VMEM((planes, 1, 128), F32),
        pltpu.VMEM((zs, 1, 128), F32),
        pltpu.SemaphoreType.DMA((4,)),
        pltpu.SemaphoreType.DMA((copies_in_all,)),
        pltpu.SemaphoreType.DMA((copies_in_all,)),
    ]
    hbm = pl.BlockSpec(memory_space=pltpu.HBM)
    vmem = pl.BlockSpec(memory_space=pltpu.VMEM)
    smem = pl.BlockSpec(memory_space=pltpu.SMEM)
    return pl.pallas_call(
        kernel,
        out_shape=(
            jax.ShapeDtypeStruct(unit, F32),
            jax.ShapeDtypeStruct(unit, F32),
            jax.ShapeDtypeStruct((3,), F32),
        ),
        in_specs=[hbm, hbm, smem, smem, smem],
        out_specs=(vmem, vmem, smem),
        scratch_shapes=scratch,
        compiler_params=pltpu.CompilerParams(
            collective_id=0, has_side_effects=True
        ),
    )


def solution(mesh):
    sizes = (4, 2, 4, 4, 2)
    split = Mesh(mesh.devices.reshape(sizes), AXES)

    def local(points, right_side, lengthscale, outputscale, noise_level):
        columns, width = right_side.shape
        call = make_kernel(sizes, columns, width, width * math.prod(sizes))
        return call(points, right_side, lengthscale, outputscale, noise_level)

    return jax.shard_map(
        local,
        mesh=split,
        in_specs=(P(None, AXES), P(None, AXES), P(), P(), P()),
        out_specs=(P(None, AXES), P(None, AXES), P()),
        check_vma=False,
    )
```

```python
import math

import jax
import jax.numpy as jnp
from jax import lax
from jax.experimental import pallas as pl
from jax.experimental.pallas import tpu as pltpu
from jax.sharding import Mesh
from jax.sharding import PartitionSpec as P

AXES = ("x", "zl", "y", "zh", "c")
BY_ID = pl.DeviceIdType.MESH
F32 = jnp.float32
BF16 = jnp.bfloat16
FEATURES = 64
UNIT = 80


def add_all(terms):
    total = terms[0]
    for term in terms[1:]:
        total = total + term
    return total


def two_sum(a, b):
    s = a + b
    t = s - a
    return s, (a - (s - t)) + (b - t)


def pair_sum(a, b):
    s, e = two_sum(a[0], b[0])
    e = e + (a[1] + b[1])
    high = s + e
    return high, e - (high - s)


def halves(a):
    t = a * 4097.0
    high = t - (t - a)
    return high, a - high


def two_product(a, b):
    p = a * b
    (ah, al), (bh, bl) = halves(a), halves(b)
    return p, ((ah * bh - p) + ah * bl + al * bh) + al * bl


def pair_tree(pairs):
    while len(pairs) > 1:
        pairs = [pair_sum(pairs[i], pairs[i + 1]) for i in range(0, len(pairs), 2)]
    return pairs[0]


def make_kernel(sizes, columns, width, total_points):
    xs, zls, ys, zhs, cs = sizes
    zs, gs = zls * zhs, ys * cs
    planes = xs * gs
    half = zs // 2
    x_tiles, row_tiles = zs // 2, gs // 2
    tiles = xs * x_tiles
    wide = 2 * width
    copies_in_all = 3 * (zs - 1) + 5 * (gs - 1) + 18 + 2 * (planes - 1 + zs - 1)
    z_offsets = [0] + [k for d in range(1, half) for k in (d, zs - d)] + [half]

    def kernel(
        points_in,
        right_in,
        length_in,
        scale_in,
        noise_in,
        solution_out,
        residual_out,
        gradient_out,
        cols,
        r0c,
        a1c,
        rows,
        r0r,
        a1r,
        d2r,
        weights,
        kmat,
        gmat,
        acc,
        vb2,
        upright,
        rs1,
        rs2,
        plane1,
        line1,
        plane2,
        line2,
        local_sems,
        send_sems,
        recv_sems,
    ):
        x, y, c = lax.axis_index("x"), lax.axis_index("y"), lax.axis_index("c")
        z = lax.axis_index("zh") * zls + lax.axis_index("zl")

        def z_peer(k):
            to = lax.rem(z + k, zs)
            return {"zl": lax.rem(to, zls), "zh": lax.div(to, zls)}

        def plane_peer(s):
            dx, dy, dc = s // gs, s % gs // cs, s % cs
            return {"x": lax.rem(x + dx, xs), "y": lax.rem(y + dy, ys), "c": lax.rem(c + dc, cs)}

        def x_peer(k):
            return {"x": lax.rem(x + k, xs)}

        barrier = pltpu.get_barrier_semaphore()
        peers = [z_peer(k) for k in range(1, zs)] + [plane_peer(s) for s in range(1, planes)]
        for peer in peers:
            pl.semaphore_signal(barrier, inc=1, device_id=peer, device_id_type=BY_ID)

        fetches = [
            pltpu.make_async_copy(src, dst, local_sems.at[i])
            for i, (src, dst) in enumerate(
                [
                    (right_in, r0c.at[0, 0]),
                    (right_in, r0r.at[0]),
                    (points_in, cols.at[0, 0, pl.ds(0, FEATURES)]),
                    (points_in, rows.at[0]),
                ]
            )
        ]
        for fetch in fetches:
            fetch.start()
        started = []

        def send(src, dst, device):
            index = len(started)
            copy = pltpu.make_async_remote_copy(
                src_ref=src,
                dst_ref=dst,
                send_sem=send_sems.at[index],
                recv_sem=recv_sems.at[index],
                device_id=device,
                device_id_type=BY_ID,
            )
            copy.start()
            started.append(copy)
            return copy

        def to_z(src, slots):
            return [send(src, slots(j), z_peer(z_offsets[j])) for j in range(1, zs)]

        def to_g(src, slots):
            return [send(src, slots(s), plane_peer(s)) for s in range(1, gs)]

        def opposite(s):
            return ((ys - s // cs) % ys) * cs + s % cs

        def wait(copies):
            for copy in copies:
                copy.wait_recv()

        acc[...] = jnp.zeros_like(acc)
        for r in range(row_tiles):
            weights[r, UNIT:128, :] = jnp.zeros((128 - UNIT, wide), BF16)
        for fetch in fetches:
            fetch.wait()
        r0 = r0c[0, 0]
        cols[0, 0, FEATURES:UNIT, :] = r0.astype(BF16)
        pl.semaphore_wait(barrier, len(peers))

        z_cols = to_z(cols.at[0, 0], lambda j: cols.at[0, j])
        g_rows = to_g(rows.at[0], lambda s: rows.at[s])
        inv = jnp.max(1.0 / jnp.full((8, 128), length_in[0], F32))
        root = inv * math.sqrt(5.0)
        rate = inv * (-math.sqrt(5.0) / math.log(2.0))
        third = inv * inv * (5.0 / 3.0)
        amplitude, jitter = scale_in[0], noise_in[0]

        line = lax.broadcasted_iota(jnp.int32, (16, width), 0)
        first, second = line < 3, (line >= 3) & (line < 6)

        def norm_pieces(values):
            norm = jnp.sum(values * values, axis=0, keepdims=True)
            high = norm.astype(BF16).astype(F32)
            middle = (norm - high).astype(BF16).astype(F32)
            low = norm - high - middle
            return jnp.where(line % 3 == 0, high, jnp.where(line % 3 == 1, middle, low))

        def column_side(unit):
            values = unit.astype(F32)
            extra = jnp.where(first, norm_pieces(values), jnp.where(second, 1.0, 0.0))
            padding = jnp.zeros((128 - UNIT, width), F32)
            return jnp.transpose(jnp.concatenate([values, extra, padding], axis=0)).astype(BF16)

        def row_side(unit):
            values = unit.astype(F32)
            extra = jnp.where(first, 1.0, jnp.where(second, norm_pieces(values), 0.0))
            return jnp.concatenate([values * -2.0, extra], axis=0).astype(BF16)

        def kernel_pair(inner):
            dist = jnp.maximum(inner, 1e-30)
            root_dist = dist * lax.rsqrt(dist)
            damping = jnp.exp2(root_dist * rate)
            linear = root_dist * root + 1.0
            bend = dist * third
            plain = linear * damping
            return (plain + bend * damping).astype(BF16), (bend * plain * inv).astype(BF16)

        def add_product(part, r, product):
            acc[part, 2 * r] += product[:, :width]
            acc[part, 2 * r + 1] += product[:, width:]

        def load_tile(slot, t):
            turned = [column_side(cols[slot, 2 * t + h, 0:FEATURES, :]) for h in range(2)]
            vectors = [cols[slot, 2 * t + h, FEATURES:UNIT, :] for h in range(2)]
            return jnp.concatenate(turned, axis=0), jnp.concatenate(vectors, axis=1)

        def one_block(at, r, turned, vectors):
            inner = jnp.dot(turned, weights[r], preferred_element_type=F32)
            for q in range(0, wide, 32):
                kern, dkern = kernel_pair(inner[q : q + 32])
                kmat[r, at, q : q + 32, :] = kern
                gmat[r, at, q : q + 32, :] = dkern
            add_product(0, r, jnp.dot(vectors, kmat[r, at], preferred_element_type=F32))
            add_product(1, r, jnp.dot(vectors, gmat[r, at], preferred_element_type=F32))

        def sweep(slot, low_tile, high_tile):
            def one_tile(t, carry):
                turned, vectors = load_tile(slot, t)
                for r in range(row_tiles):
                    one_block(slot * x_tiles + t, r, turned, vectors)
                return carry

            lax.fori_loop(low_tile, high_tile, one_tile, 0)

        def ring_send(buf, h, slot, way):
            part = pl.ds(h * half, half)
            return [send(buf.at[0, part], buf.at[slot, part], x_peer(way))]

        def ring_rest(buf, ring):
            ring["right", 1] = ring_send(buf, 1, 1, 1)
            ring["left", 1] = ring_send(buf, 1, 2, xs - 1)
            ring["left", 0] = ring_send(buf, 0, 2, xs - 1)

        def pass_right(buf, ring):
            wait(ring["right", 0])
            part = pl.ds(0, half)
            ring["far", 0] = [send(buf.at[1, part], buf.at[3, part], x_peer(1))]

        def pass_left(buf, ring):
            wait(ring["left", 1])
            part = pl.ds(half, half)
            ring["far", 1] = [send(buf.at[2, part], buf.at[3, part], x_peer(xs - 1))]

        mid = x_tiles // 2
        wait(g_rows)
        for r in range(row_tiles):
            weights[r, 0:UNIT, :] = jnp.concatenate([row_side(rows[2 * r]), row_side(rows[2 * r + 1])], axis=1)
        ring = {}
        wait(z_cols[: half - 1])
        ring["right", 0] = ring_send(cols, 0, 1, 1)
        sweep(0, 0, mid)
        wait(z_cols[half - 1 :])
        ring_rest(cols, ring)
        z_r0 = to_z(r0c.at[0, 0], lambda j: r0c.at[0, j])
        g_r0 = to_g(r0r.at[0], lambda s: r0r.at[s])
        sweep(0, mid, x_tiles)
        pass_right(cols, ring)
        sweep(1, 0, mid)
        pass_left(cols, ring)
        sweep(2, mid, x_tiles)
        wait(ring["right", 1])
        sweep(1, mid, x_tiles)
        wait(ring["left", 0])
        sweep(2, 0, mid)
        wait(ring["far", 0])
        sweep(3, 0, mid)
        wait(ring["far", 1])
        wait(z_r0)
        ring0 = {("right", 0): ring_send(r0c, 0, 1, 1)}
        ring_rest(r0c, ring0)

        order = [r for r in range(1, row_tiles)] + [0]
        loaded = [load_tile(3, t) for t in range(mid, x_tiles)]
        arriving = []
        for r in order:
            for t in range(mid, x_tiles):
                one_block(3 * x_tiles + t, r, *loaded[t - mid])
            for s in (2 * r, 2 * r + 1):
                if s:
                    arriving.append(send(acc.at[0, s], rs1.at[opposite(s)], plane_peer(opposite(s))))
        wait(arriving)
        product = add_all([acc[0, 0]] + [rs1[s] for s in range(1, gs)])
        a1 = amplitude * product + jitter * r0
        a1c[0, 0] = a1
        a1r[0] = a1
        z_a1 = to_z(a1c.at[0, 0], lambda j: a1c.at[0, j])
        g_a1 = to_g(a1r.at[0], lambda s: a1r.at[s])

        lane = lax.broadcasted_iota(jnp.int32, (8, 128), 1)

        def stack(parts):
            parts = list(parts) + [jnp.zeros((128 - columns * len(parts), width), F32)] * (columns * len(parts) < 128)
            return jnp.transpose(jnp.concatenate(parts, axis=0))

        def unstack(row):
            turned = jnp.transpose(jnp.broadcast_to(row[0:1], (128, 128)))
            return [turned[columns * i : columns * (i + 1)] for i in range(128 // columns)]

        def sublane_pair(pair):
            for shift in (4, 2, 1):
                pair = pair_sum(pair, tuple(pltpu.roll(v, shift, 0) for v in pair))
            return pair

        def join(pair):
            return jnp.where(lane < 64, pair[0], pltpu.roll(pair[1], 64, 1))

        def split(row):
            return row, pltpu.roll(row, 64, 1)

        def eights(buf, count):
            return [jnp.concatenate([buf[i + j] for j in range(8)], axis=0) for i in range(0, count, 8)]

        def pair_total(buf, count):
            return sublane_pair(pair_tree([split(rows8) for rows8 in eights(buf, count)]))

        products = [two_product(r0, r0), two_product(r0, a1), two_product(a1, a1)]
        high, low = stack([p for p, _ in products]), stack([e for _, e in products])
        own_sums = sublane_pair(pair_tree([(high[i : i + 8], low[i : i + 8]) for i in range(0, 128, 8)]))
        plane1[0] = join(own_sums)[0:1]
        in_plane = [send(plane1.at[0], plane1.at[s], plane_peer(s)) for s in range(1, planes)]

        pass_right(r0c, ring0)
        pass_left(r0c, ring0)
        ring = {}
        wait(z_a1[: half - 1])
        ring["right", 0] = ring_send(a1c, 0, 1, 1)
        wait(z_a1[half - 1 :])
        ring_rest(a1c, ring)
        wait(in_plane)
        line1[0] = join(pair_total(plane1, planes))[0:1]
        in_line = [send(line1.at[0], line1.at[k], z_peer(k)) for k in range(1, zs)]
        pass_right(a1c, ring)
        pass_left(a1c, ring)
        wait(g_a1 + g_r0)
        wait(ring0["right", 1] + ring0["left", 0] + ring0["far", 0] + ring0["far", 1])
        wait(in_line)
        sums = pair_total(line1, zs)

        def aligned(i):
            return tuple(pltpu.roll(v, (128 - columns * i) % 128, 1) if i else v for v in sums)

        rr0_pair, curve_pair, aa_pair = aligned(0), aligned(1), aligned(2)
        step1_row = rr0_pair[0] / curve_pair[0]
        cross, cross_low = two_product(curve_pair[0], -2.0 * step1_row)
        cross = (cross, cross_low - 2.0 * step1_row * curve_pair[1])
        square, square_low = two_product(step1_row, step1_row)
        bend, bend_low = two_product(aa_pair[0], square)
        bend = (bend, bend_low + (aa_pair[0] * square_low + aa_pair[1] * square))
        rr1_pair = pair_sum(pair_sum(rr0_pair, cross), bend)
        rr1_row = rr1_pair[0] + rr1_pair[1]
        packed = step1_row
        for i, row in enumerate((rr1_row / rr0_pair[0], rr1_row, rr0_pair[0])):
            packed = jnp.where(lane >= columns * (i + 1), pltpu.roll(row, columns * (i + 1), 1), packed)
        step1, ratio, rr1, rr0 = unstack(packed)[:4]
        wait(ring["right", 1] + ring["left", 0] + ring["far", 0] + ring["far", 1])

        def new_direction(r0_part, a1_part):
            return (r0_part - step1 * a1_part) + ratio * r0_part

        for i in range(xs):
            for t in range(x_tiles):
                pair = [new_direction(r0c[i, 2 * t + h], a1c[i, 2 * t + h]) for h in range(2)]
                at = i * x_tiles + t
                side, place = at // (tiles // 2), at % (tiles // 2) * wide
                vb2[side, :, place : place + wide] = jnp.concatenate(pair, axis=1).astype(BF16)
                for h in range(2):
                    upright[i * x_tiles + t, h * width : (h + 1) * width, :] = jnp.transpose(
                        jnp.broadcast_to(pair[h][0:1], (width, width))
                    )
        for s in range(gs):
            d2r[s] = new_direction(r0r[s], a1r[s])
        d2 = d2r[0]

        arriving = []
        bilinear = jnp.zeros((16, width), F32)
        for both in zip(order[::2], order[1::2]):
            totals, slopes = {}, {r: jnp.zeros((16, wide), F32) for r in both}
            for t in range(tiles):
                side, place = t // (tiles // 2), t % (tiles // 2) * wide
                vectors = vb2[side, :, place : place + wide]
                for r in both:
                    product = jnp.dot(vectors, kmat[r, t], preferred_element_type=F32)
                    totals[r] = totals[r] + product if r in totals else product
                for r in both:
                    for q in range(0, wide, 64):
                        scale = upright[t, q : q + 64, :]
                        terms = gmat[r, t, q : q + 64, :].astype(F32) * jnp.concatenate([scale, scale], axis=1)
                        slopes[r] = slopes[r] + add_all([terms[i : i + 16] for i in range(0, 64, 16)])
            for r in both:
                for h in range(2):
                    s = 2 * r + h
                    acc[2, s] = totals[r][:, h * width : (h + 1) * width]
                    bilinear = bilinear + slopes[r][:, h * width : (h + 1) * width] * d2r[s][0:1]
                    if s:
                        arriving.append(send(acc.at[2, s], rs2.at[opposite(s)], plane_peer(opposite(s))))

        def dot_rows(left, part):
            return add_all([left[s] * acc[part, s] for s in range(gs)])

        top = lax.broadcasted_iota(jnp.int32, (columns, width), 0) == 0
        slope_rows = jnp.where(top, jnp.sum(bilinear, axis=0, keepdims=True), 0.0)
        stats = [dot_rows(r0r, 0), dot_rows(r0r, 1), dot_rows(d2r, 1), slope_rows]
        stats += [dot_rows(r0r, 2), dot_rows(d2r, 2), r0 * d2, d2 * d2]
        plane2[0] = jnp.sum(stack(stats), axis=0, keepdims=True)
        wait([send(plane2.at[0], plane2.at[s], plane_peer(s)) for s in range(1, planes)])
        line2[0] = jnp.sum(add_all(eights(plane2, planes)), axis=0, keepdims=True)
        wait([send(line2.at[0], line2.at[k], z_peer(k)) for k in range(1, zs)])
        total = jnp.sum(add_all(eights(line2, zs)), axis=0, keepdims=True)
        r0_k1, r0_g1, d2_g1, d2_g2, r0_k2, d2_k2, r0_d2, d2_d2 = unstack(total)

        step2 = rr1 / (amplitude * d2_k2 + jitter * d2_d2)
        wait(arriving)
        product = add_all([acc[2, 0]] + [rs2[s] for s in range(1, gs)])
        applied = amplitude * product + jitter * d2
        solution_out[...] = step1 * r0 + step2 * d2
        residual_out[...] = (r0 - step1 * a1) - step2 * applied

        weight = jnp.where(top, 1.0, -1.0 / (columns - 1))

        def quadratic(r0_r0, mixed, d2_d2):
            plain = step1 * r0_r0 + step2 * mixed
            other = step1 * mixed + step2 * d2_d2
            terms = weight * jnp.where(top, step1 * plain + step2 * other, plain)
            return jnp.sum(terms[:, 0:1])

        share = 0.5 / total_points
        gradient_out[0] = quadratic(r0_g1, d2_g1, d2_g2) * amplitude * share
        gradient_out[1] = quadratic(r0_k1, r0_k2, d2_k2) * share
        gradient_out[2] = quadratic(rr0, r0_d2, d2_d2) * share

        assert len(started) == copies_in_all, len(started)
        for copy in started:
            copy.wait_send()

    unit = (columns, width)
    scratch = [
        pltpu.VMEM((xs, zs, UNIT, width), BF16),
        pltpu.VMEM((xs, zs, *unit), F32),
        pltpu.VMEM((xs, zs, *unit), F32),
        pltpu.VMEM((gs, FEATURES, width), BF16),
        pltpu.VMEM((gs, *unit), F32),
        pltpu.VMEM((gs, *unit), F32),
        pltpu.VMEM((gs, *unit), F32),
        pltpu.VMEM((row_tiles, 128, wide), BF16),
        pltpu.VMEM((row_tiles, tiles, wide, wide), BF16),
        pltpu.VMEM((row_tiles, tiles, wide, wide), BF16),
        pltpu.VMEM((3, gs, *unit), F32),
        pltpu.VMEM((2, columns, tiles // 2 * wide), BF16),
        pltpu.VMEM((tiles, wide, width), F32),
        pltpu.VMEM((gs, *unit), F32),
        pltpu.VMEM((gs, *unit), F32),
        pltpu.VMEM((planes, 1, 128), F32),
        pltpu.VMEM((zs, 1, 128), F32),
        pltpu.VMEM((planes, 1, 128), F32),
        pltpu.VMEM((zs, 1, 128), F32),
        pltpu.SemaphoreType.DMA((4,)),
        pltpu.SemaphoreType.DMA((copies_in_all,)),
        pltpu.SemaphoreType.DMA((copies_in_all,)),
    ]
    hbm = pl.BlockSpec(memory_space=pltpu.HBM)
    vmem = pl.BlockSpec(memory_space=pltpu.VMEM)
    smem = pl.BlockSpec(memory_space=pltpu.SMEM)
    return pl.pallas_call(
        kernel,
        out_shape=(
            jax.ShapeDtypeStruct(unit, F32),
            jax.ShapeDtypeStruct(unit, F32),
            jax.ShapeDtypeStruct((3,), F32),
        ),
        in_specs=[hbm, hbm, smem, smem, smem],
        out_specs=(vmem, vmem, smem),
        scratch_shapes=scratch,
        compiler_params=pltpu.CompilerParams(
            collective_id=0, has_side_effects=True
        ),
    )


def solution(mesh):
    sizes = (4, 2, 4, 4, 2)
    split = Mesh(mesh.devices.reshape(sizes), AXES)

    def local(points, right_side, lengthscale, outputscale, noise_level):
        columns, width = right_side.shape
        call = make_kernel(sizes, columns, width, width * math.prod(sizes))
        return call(points, right_side, lengthscale, outputscale, noise_level)

    return jax.shard_map(
        local,
        mesh=split,
        in_specs=(P(None, AXES), P(None, AXES), P(), P(), P()),
        out_specs=(P(None, AXES), P(None, AXES), P()),
        check_vma=False,
    )
```
